32 devices in a mesh: band: 8 (over y, x, core), gslab: 4 (over z).
Axes of the slice: x: 2, y: 2, z: 4, core: 2. Of those that a mesh axis runs over, the one named last changes fastest.
Arguments:
- band_coeffs: float32 [3072, 49152], P('band', 'gslab'), may hold values from -6 to 6
- sign_table: int32 [12, 3072], P(None, 'band'), may hold values from -1 to 1, as said below
- slice_widths: int32 [16], replicated, may hold values from 96 to 384, as said below
- owner_map: int32 [16], replicated, may hold values from 0 to 15, each once
Outputs:
- pseudobands: float32 [192, 49152], P(('band', 'gslab'))
The draws below stay inside these ranges and needn't reach their ends.
Inputs may be any that keep to these rules, and one draw needn't show every extreme that they name: `sign_table`: every entry is -1 or 1. `slice_widths`: the widths sum to 3072; every slice holds 96 to 384 bands, and in every draw some slice holds exactly 96 and some exactly 384. `owner_map`: each slice appears once.
All inputs are finite; a program needn't handle non-finite values.
Results may differ from the reference program's by a relative error of at most 0.0003.
Values sent between devices are 32-bit elements; how exact they have to be, the bound alone decides.
A program may use at most 128 MiB of HBM per device.

```python
import jax
import jax.numpy as jnp
from jax import lax

NG = 49152
BANDS_DEV = 384
SLICE_BAND = 2
NPS = 12
NB = 3072
NSLICE = 16
MOST = 384
NPB = 192


def draw_sign_table(key, part):
    return (2 * jax.random.randint(jax.random.fold_in(key, 17), (NPS, NB), 0, 2) - 1).astype(jnp.int32)


def draw_slice_widths(key, part):
    average = BANDS_DEV // SLICE_BAND
    narrow = average // 2
    place = jax.random.randint(jax.random.fold_in(key, 3), (), 0, NSLICE - 3)
    positions = jnp.arange(NSLICE, dtype=jnp.int32)
    relative = positions - place
    special = (relative >= 0) & (relative < 4)
    ranking = jnp.where(positions < place, positions, positions - 4)
    ranking = jnp.maximum(ranking, 0)
    pair_id = jnp.minimum(ranking // 2, NSLICE // 2 - 1)
    parity = ranking % 2
    spread = jax.random.randint(jax.random.fold_in(key, 5), (NSLICE // 2,), -(average - narrow), average - narrow + 1)
    shift_value = spread[pair_id]
    drawn = average + jnp.where(parity == 0, shift_value, -shift_value)
    table = jnp.array([narrow, 2 * average, narrow, average], dtype=jnp.int32)
    marked = table[jnp.clip(relative, 0, 3)]
    return jnp.where(special, marked, drawn).astype(jnp.int32)


def block_levels(key, extent, split, low, largest):
    level, own = 1.0, jax.random.fold_in(key, 6)
    for position, blocks in split:
        draws = jnp.exp(jax.random.uniform(jax.random.fold_in(own, position), (blocks,), jnp.float32, low / len(split), largest / len(split)))
        level = level * jnp.repeat(draws, extent[position] // blocks).reshape([-1 if axis == position else 1 for axis in range(len(extent))])
    return level


def centred(rng, shape, width, most, split=(), kind=jnp.bfloat16):
    values = width * jax.random.normal(rng, shape, jnp.float32)
    if split:
        values = values * block_levels(rng, shape, split, -0.22, 0.18)
    return jnp.clip(values, -most, most).astype(kind)


def setup_inputs(seed: int = 0) -> dict:
    key_of = jax.random.split(jax.random.key(seed), 5)
    return {
        "band_coeffs": centred(key_of[0], (NB, NG), 1.0, 6.0, ((0, 8), (1, 4)), jnp.float32),
        "sign_table": draw_sign_table(jax.random.fold_in(key_of[4], 71), 0),
        "slice_widths": draw_slice_widths(jax.random.fold_in(key_of[4], 71), 0),
        "owner_map": jax.random.permutation(key_of[3], NSLICE).astype(jnp.int32),
    }


def reference(band_coeffs, sign_table, slice_widths, owner_map):
    ends = jnp.cumsum(slice_widths).astype(jnp.int32)
    starts = (ends - slice_widths).astype(jnp.int32)
    inverse = 1.0 / jnp.sqrt(slice_widths.astype(jnp.float32))

    def one_slice(slice_id):
        begin = starts[slice_id]
        finish = ends[slice_id]
        window_start = jnp.minimum(begin, NB - MOST).astype(jnp.int32)
        block = lax.dynamic_slice(band_coeffs, (window_start, jnp.int32(0)), (MOST, NG))
        band_ids = window_start + jnp.arange(MOST, dtype=jnp.int32)
        inside = (band_ids >= begin) & (band_ids < finish)
        sign_block = lax.dynamic_slice(sign_table, (jnp.int32(0), window_start), (NPS, MOST)).astype(jnp.float32)
        weights = jnp.where(inside[None, :], sign_block * inverse[slice_id], jnp.zeros_like(sign_block))
        return jnp.dot(weights, block, precision=lax.Precision.HIGHEST, preferred_element_type=jnp.float32)
    result = lax.map(one_slice, jnp.arange(NSLICE, dtype=jnp.int32))
    return result[owner_map].reshape(NPB, NG)
```

```python
import functools

import jax
import jax.numpy as jnp
from jax import lax
from jax.experimental import pallas as pl
from jax.experimental.pallas import tpu as pltpu
from jax.sharding import PartitionSpec as P

NARROWEST = 96
LANES = 128
AHEAD = 4
MESH = pl.DeviceIdType.MESH


def mixing_rows(row_ids, slice_of_band, sign_float, owner_map, inverse, per_slice):
    slice_count = owner_map.shape[0]
    slot_group = row_ids // per_slice
    within = row_ids % per_slice
    slice_range = jnp.arange(slice_count, dtype=jnp.int32)
    picked = slot_group[:, None] == slice_range[None, :]
    target = jnp.sum(jnp.where(picked, owner_map[None, :], 0), axis=1)
    member = target[:, None] == slice_range[None, :]
    row_scale = jnp.sum(jnp.where(member, inverse[None, :], 0.0), axis=1)
    one_hot = (within[:, None] == jnp.arange(per_slice, dtype=jnp.int32)[None, :]).astype(
        jnp.float32
    )
    sign_rows = jnp.dot(
        one_hot, sign_float, precision=lax.Precision.HIGHEST, preferred_element_type=jnp.float32
    )
    return jnp.where(slice_of_band[None, :] == target[:, None], sign_rows * row_scale[:, None], 0.0)


def dense(band_coeffs, sign_table, slice_widths, owner_map):
    local_bands = band_coeffs.shape[0]
    per_slice = sign_table.shape[0]
    slice_count = owner_map.shape[0]
    total_rows = slice_count * per_slice
    first_band = lax.axis_index("band") * local_bands
    band_ids = first_band + jnp.arange(local_bands, dtype=jnp.int32)
    ends = jnp.cumsum(slice_widths)
    slice_of_band = jnp.sum((band_ids[:, None] >= ends[None, :]).astype(jnp.int32), axis=1)
    inverse = 1.0 / jnp.sqrt(slice_widths.astype(jnp.float32))
    sign_float = sign_table.astype(jnp.float32)
    row_ids = jnp.arange(total_rows, dtype=jnp.int32)
    mixing = mixing_rows(row_ids, slice_of_band, sign_float, owner_map, inverse, per_slice)
    summed = lax.psum_scatter(
        jnp.dot(
            mixing, band_coeffs, precision=lax.Precision.HIGHEST, preferred_element_type=jnp.float32
        ),
        "band",
        scatter_dimension=0,
        tiled=True,
    )
    return lax.all_to_all(summed, "gslab", split_axis=0, concat_axis=1, tiled=True)


def two_term_dot(exact, values):
    high = values.astype(jnp.bfloat16)
    low = (values - high.astype(jnp.float32)).astype(jnp.bfloat16)
    return jnp.dot(exact, high, preferred_element_type=jnp.float32) + jnp.dot(
        exact, low, preferred_element_type=jnp.float32
    )


def kernel(
    groups, slabs, pieces, reach,
    widths_ref, owner_ref, signs_ref, band_ref, out_ref,
    held, mix, sent, got, chosen, scale, done,
    load_sem, send1, recv1, send2, recv2,
):
    devices = groups * slabs
    my_group = lax.axis_index("band")
    my_slab = lax.axis_index("gslab")
    me = my_group * slabs + my_slab
    per_slice, local_bands = signs_ref.shape
    slices = widths_ref.shape[0]
    packed, width = sent.shape[2:]
    mine = done.shape[2]
    slot = chosen.shape[0] // devices
    total = groups * pieces

    def load(step):
        part = step // groups
        group = lax.rem(my_group + 1 + lax.rem(step, groups), groups)
        index = group * pieces + part
        return pltpu.make_async_copy(
            band_ref.at[:, pl.ds(pl.multiple_of(index * width, width), width)],
            held.at[index],
            load_sem.at[index],
        )

    for step in range(AHEAD):
        load(step).start()

    barrier = pltpu.get_barrier_semaphore()

    @pl.loop(1, devices)
    def _(k):
        other = lax.rem(me + k, devices)
        pl.semaphore_signal(
            barrier, inc=1,
            device_id={"band": other // slabs, "gslab": lax.rem(other, slabs)},
            device_id_type=MESH,
        )

    ends = []
    running = jnp.int32(0)
    for s in range(slices):
        running = running + widths_ref[s]
        ends.append(running)

    first_band = my_group * local_bands
    bands = first_band + lax.broadcasted_iota(jnp.int32, (1, local_bands), 1)
    slice_of = jnp.zeros((1, local_bands), jnp.int32)
    first = jnp.int32(0)
    for s in range(slices):
        slice_of = slice_of + jnp.where(bands >= ends[s], 1, 0)
        first = first + jnp.where(first_band >= ends[s], 1, 0)
    row = lax.broadcasted_iota(jnp.int32, (packed, per_slice), 0)
    column = lax.broadcasted_iota(jnp.int32, (packed, per_slice), 1)
    repeat = jnp.where(lax.rem(row, per_slice) == column, 1.0, 0.0).astype(jnp.float32)
    signs = jnp.dot(
        repeat, signs_ref[...].astype(jnp.float32), preferred_element_type=jnp.float32
    )
    row = lax.broadcasted_iota(jnp.int32, (packed, local_bands), 0)
    hit = (slice_of - first == row // per_slice) & (row < reach * per_slice)
    mix[...] = jnp.where(hit, signs, 0.0).astype(jnp.bfloat16)

    def exchange(group, source, part):
        return pltpu.make_async_remote_copy(
            src_ref=sent.at[part, group],
            dst_ref=got.at[part, source],
            send_sem=send1.at[part, group],
            recv_sem=recv1.at[part, source],
            device_id={"band": group, "gslab": my_slab},
            device_id_type=MESH,
        )

    def partial_sums(part, k):
        step = part * groups + k
        load(step).wait()

        @pl.when(step + AHEAD < total)
        def _():
            load(step + AHEAD).start()

        group = lax.rem(my_group + 1 + k, groups)
        return group, two_term_dot(mix[...], held[group * pieces + part])

    def send_partial(part):
        @pl.loop(0, groups - 1)
        def _(k):
            group, value = partial_sums(part, k)
            sent[part, group] = value
            exchange(group, my_group, part).start()

        _, value = partial_sums(part, groups - 1)
        got[part, my_group] = value

    def columns(group, slab, part):
        start = slab * (total * width) + (group * pieces + part) * width
        return out_ref.at[:, pl.ds(pl.multiple_of(start, width), width)]

    def deliver(other, source, part):
        return pltpu.make_async_remote_copy(
            src_ref=done.at[part, other],
            dst_ref=columns(source // slabs, lax.rem(source, slabs), part),
            send_sem=send2.at[part, other],
            recv_sem=recv2.at[part, source],
            device_id={"band": other // slabs, "gslab": lax.rem(other, slabs)},
            device_id_type=MESH,
        )

    def keep(part):
        return pltpu.make_async_copy(
            done.at[part, me], columns(my_group, my_slab, part), recv2.at[part, me]
        )

    def finish(part):
        @pl.loop(1, groups)
        def _(k):
            source = lax.rem(my_group + k, groups)
            exchange(source, source, part).wait_recv()

        rows = got[part].reshape(groups * packed, width)
        value = two_term_dot(chosen[...], rows) * scale[:, :1]
        done[part] = value.reshape(devices, slot, width)[:, :mine]
        keep(part).start()

        @pl.loop(1, devices)
        def _(k):
            deliver(lax.rem(me + k, devices), me, part).start()

    pl.semaphore_wait(barrier, devices - 1)
    send_partial(0)

    shape = (devices * slot, 1)
    tall = lax.broadcasted_iota(jnp.int32, shape, 0)
    within = lax.rem(tall, slot)
    output_row = (tall // slot) * mine + within
    block = output_row // per_slice
    target = jnp.zeros(shape, jnp.int32)
    for s in range(slices):
        target = jnp.where(block == s, owner_ref[s], target)
    breadth = jnp.ones(shape, jnp.int32)
    for s in range(slices):
        breadth = jnp.where(target == s, widths_ref[s], breadth)
    scale[...] = jnp.broadcast_to(1.0 / jnp.sqrt(breadth.astype(jnp.float32)), scale.shape)
    wanted = jnp.where(within < mine, target * per_slice + lax.rem(output_row, per_slice), -1)
    wide = lax.broadcasted_iota(jnp.int32, (1, groups * packed), 1)
    place = lax.rem(wide, packed)
    begin = (wide // packed) * local_bands
    lowest = jnp.zeros((1, groups * packed), jnp.int32)
    for s in range(slices):
        lowest = lowest + jnp.where(begin >= ends[s], 1, 0)
    offered = jnp.where(place < reach * per_slice, lowest * per_slice + place, -2)
    chosen[...] = jnp.where(wanted == offered, 1.0, 0.0).astype(jnp.bfloat16)

    for part in range(1, pieces):
        send_partial(part)
        finish(part - 1)
    finish(pieces - 1)

    for part in range(pieces):
        @pl.loop(1, groups)
        def _(k):
            exchange(lax.rem(my_group + k, groups), my_group, part).wait_send()

        @pl.loop(1, devices)
        def _(k):
            other = lax.rem(me + k, devices)
            deliver(other, other, part).wait()

        keep(part).wait()


def on_device(groups, slabs, band_coeffs, sign_table, slice_widths, owner_map):
    local_bands, local_columns = band_coeffs.shape
    per_slice = sign_table.shape[0]
    rows = owner_map.shape[0] * per_slice
    devices = groups * slabs
    share, odd = divmod(local_columns, groups * LANES)
    if odd or rows % devices:
        return dense(band_coeffs, sign_table, slice_widths, owner_map)
    pieces = next(p for p in (3, 4, 2, 1) if share % p == 0)
    width = share // pieces * LANES
    reach = (local_bands - 2) // NARROWEST + 2
    packed = -(-reach * per_slice // 8) * 8
    mine = rows // devices
    slot = -(-mine // 8) * 8
    return pl.pallas_call(
        functools.partial(kernel, groups, slabs, pieces, reach),
        out_shape=jax.ShapeDtypeStruct((mine, local_columns * slabs), jnp.float32),
        in_specs=[
            pl.BlockSpec(memory_space=pltpu.SMEM),
            pl.BlockSpec(memory_space=pltpu.SMEM),
            pl.BlockSpec(memory_space=pltpu.VMEM),
            pl.BlockSpec(memory_space=pl.ANY),
        ],
        out_specs=pl.BlockSpec(memory_space=pl.ANY),
        scratch_shapes=[
            pltpu.VMEM((groups * pieces, local_bands, width), jnp.float32),
            pltpu.VMEM((packed, local_bands), jnp.bfloat16),
            pltpu.VMEM((pieces, groups, packed, width), jnp.float32),
            pltpu.VMEM((pieces, groups, packed, width), jnp.float32),
            pltpu.VMEM((devices * slot, groups * packed), jnp.bfloat16),
            pltpu.VMEM((devices * slot, LANES), jnp.float32),
            pltpu.VMEM((pieces, devices, mine, width), jnp.float32),
            pltpu.SemaphoreType.DMA((groups * pieces,)),
            pltpu.SemaphoreType.DMA((pieces, groups)),
            pltpu.SemaphoreType.DMA((pieces, groups)),
            pltpu.SemaphoreType.DMA((pieces, devices)),
            pltpu.SemaphoreType.DMA((pieces, devices)),
        ],
        compiler_params=pltpu.CompilerParams(
            collective_id=0, has_side_effects=True, vmem_limit_bytes=56 * 2**20
        ),
        name="pseudobands",
    )(slice_widths, owner_map, sign_table, band_coeffs)


def solution(mesh):
    return jax.shard_map(
        functools.partial(on_device, mesh.shape["band"], mesh.shape["gslab"]),
        mesh=mesh,
        in_specs=(P("band", "gslab"), P(None, "band"), P(), P()),
        out_specs=P(("band", "gslab"), None),
        check_vma=False,
    )
```

```python
import functools

import jax
import jax.numpy as jnp
from jax import lax
from jax.experimental import pallas as pl
from jax.experimental.pallas import tpu as pltpu
from jax.sharding import PartitionSpec as P

NARROWEST = 96
LANES = 128
PIECES = (8, 4, 2, 1)
MERGE_LAG = 2
FINISH_LAG = 4
MESH = pl.DeviceIdType.MESH


def mixing_rows(row_ids, slice_of_band, sign_float, owner_map, inverse, per_slice):
    slice_count = owner_map.shape[0]
    slot_group = row_ids // per_slice
    within = row_ids % per_slice
    slice_range = jnp.arange(slice_count, dtype=jnp.int32)
    picked = slot_group[:, None] == slice_range[None, :]
    target = jnp.sum(jnp.where(picked, owner_map[None, :], 0), axis=1)
    member = target[:, None] == slice_range[None, :]
    row_scale = jnp.sum(jnp.where(member, inverse[None, :], 0.0), axis=1)
    one_hot = (within[:, None] == jnp.arange(per_slice, dtype=jnp.int32)[None, :]).astype(
        jnp.float32
    )
    sign_rows = jnp.dot(
        one_hot, sign_float, precision=lax.Precision.HIGHEST, preferred_element_type=jnp.float32
    )
    return jnp.where(slice_of_band[None, :] == target[:, None], sign_rows * row_scale[:, None], 0.0)


def dense(band_coeffs, sign_table, slice_widths, owner_map):
    local_bands = band_coeffs.shape[0]
    per_slice = sign_table.shape[0]
    slice_count = owner_map.shape[0]
    total_rows = slice_count * per_slice
    first_band = lax.axis_index("band") * local_bands
    band_ids = first_band + jnp.arange(local_bands, dtype=jnp.int32)
    ends = jnp.cumsum(slice_widths)
    slice_of_band = jnp.sum((band_ids[:, None] >= ends[None, :]).astype(jnp.int32), axis=1)
    inverse = 1.0 / jnp.sqrt(slice_widths.astype(jnp.float32))
    sign_float = sign_table.astype(jnp.float32)
    row_ids = jnp.arange(total_rows, dtype=jnp.int32)
    mixing = mixing_rows(row_ids, slice_of_band, sign_float, owner_map, inverse, per_slice)
    summed = lax.psum_scatter(
        jnp.dot(
            mixing, band_coeffs, precision=lax.Precision.HIGHEST, preferred_element_type=jnp.float32
        ),
        "band",
        scatter_dimension=0,
        tiled=True,
    )
    return lax.all_to_all(summed, "gslab", split_axis=0, concat_axis=1, tiled=True)


def two_term_dot(exact, values):
    high = values.astype(jnp.bfloat16)
    low = (values - high.astype(jnp.float32)).astype(jnp.bfloat16)
    return jnp.dot(exact, high, preferred_element_type=jnp.float32) + jnp.dot(
        exact, low, preferred_element_type=jnp.float32
    )


def kernel(
    slabs, pieces, reach,
    widths_ref, owner_ref, signs_ref, band_ref, out_ref,
    held, mix, sent, got, chosen, scale, half, came, done,
    load_sem, send1, recv1, send2, recv2, send3, recv3,
):
    my_group = lax.axis_index("band")
    my_slab = lax.axis_index("gslab")
    my_core = lax.rem(my_group, 2)
    bits = (my_group // 4, lax.rem(my_group // 2, 2))
    devices = 8 * slabs
    me = my_group * slabs + my_slab
    per_slice, local_bands = signs_ref.shape
    slices = widths_ref.shape[0]
    packed, width = sent.shape[2:]
    mine = done.shape[2]
    peers = done.shape[1]
    live = reach * per_slice
    total = 4 * pieces

    def group_of(axis, along, other, core):
        return along * 4 + other * 2 + core if axis == 0 else other * 4 + along * 2 + core

    def own(axis):
        return bits[axis], bits[1 - axis]

    def quarter_at(axis, k):
        return lax.rem(own(axis)[0] * 2 + my_core + 1 + k, 4)

    def load(part, quarter):
        index = quarter * pieces + part
        return pltpu.make_async_copy(
            band_ref.at[:, pl.ds(pl.multiple_of(index * width, width), width)],
            held.at[index],
            load_sem.at[index],
        )

    def load_piece(part):
        for k in range(4):
            load(part, quarter_at(part % 2, k)).start()

    load_piece(0)
    barrier = pltpu.get_barrier_semaphore()

    @pl.loop(1, devices)
    def _(k):
        other = lax.rem(me + k, devices)
        pl.semaphore_signal(
            barrier, inc=1,
            device_id={"band": other // slabs, "gslab": lax.rem(other, slabs)},
            device_id_type=MESH,
        )

    ends = []
    running = jnp.int32(0)
    for s in range(slices):
        running = running + widths_ref[s]
        ends.append(running)

    first_band = my_group * local_bands
    bands = first_band + lax.broadcasted_iota(jnp.int32, (1, local_bands), 1)
    slice_of = jnp.zeros((1, local_bands), jnp.int32)
    first = jnp.int32(0)
    for s in range(slices):
        slice_of = slice_of + jnp.where(bands >= ends[s], 1, 0)
        first = first + jnp.where(first_band >= ends[s], 1, 0)
    row = lax.broadcasted_iota(jnp.int32, (packed, per_slice), 0)
    column = lax.broadcasted_iota(jnp.int32, (packed, per_slice), 1)
    repeat = jnp.where(lax.rem(row, per_slice) == column, 1.0, 0.0).astype(jnp.float32)
    signs = jnp.dot(
        repeat, signs_ref[...].astype(jnp.float32), preferred_element_type=jnp.float32
    )
    row = lax.broadcasted_iota(jnp.int32, (packed, local_bands), 0)
    hit = (slice_of - first == row // per_slice) & (row < live)
    mix[...] = jnp.where(hit, signs, 0.0).astype(jnp.bfloat16)

    def exchange(part, quarter, source):
        axis = part % 2
        return pltpu.make_async_remote_copy(
            src_ref=sent.at[part, quarter],
            dst_ref=got.at[part, source],
            send_sem=send1.at[part, quarter],
            recv_sem=recv1.at[part, source],
            device_id={
                "band": group_of(axis, quarter // 2, own(axis)[1], lax.rem(quarter, 2)),
                "gslab": my_slab,
            },
            device_id_type=MESH,
        )

    def partial_sums(part, quarter):
        load(part, quarter).wait()
        return two_term_dot(mix[...], held[quarter * pieces + part])

    def send_partial(part):
        if part + 1 < pieces:
            load_piece(part + 1)
        here = own(part % 2)[0] * 2 + my_core

        @pl.loop(0, 3)
        def _(k):
            quarter = quarter_at(part % 2, k)
            sent[part, quarter] = partial_sums(part, quarter)
            exchange(part, quarter, here).start()

        got[part, here] = partial_sums(part, here)

    def cross(part):
        axis = part % 2
        along, other = own(axis)
        return pltpu.make_async_remote_copy(
            src_ref=half.at[part, 0],
            dst_ref=came.at[part],
            send_sem=send2.at[part],
            recv_sem=recv2.at[part],
            device_id={"band": group_of(axis, along, 1 - other, my_core), "gslab": my_slab},
            device_id_type=MESH,
        )

    def merge(part):
        axis = part % 2

        @pl.loop(0, 3)
        def _(k):
            source = quarter_at(axis, k)
            exchange(part, source, source).wait_recv()

        rows = got[part].reshape(4 * packed, width)
        value = two_term_dot(chosen[axis], rows)
        half[part] = value.reshape(2, peers * mine, width)
        cross(part).start()

    def here_of(axis):
        return (own(axis)[0] * 2 + my_core) * slabs + my_slab

    def columns(part, peer):
        start = lax.rem(peer, slabs) * (total * width) + ((peer // slabs) * pieces + part) * width
        return out_ref.at[:, pl.ds(pl.multiple_of(start, width), width)]

    def deliver(part, peer, source):
        axis = part % 2
        quarter = peer // slabs
        return pltpu.make_async_remote_copy(
            src_ref=done.at[part, peer],
            dst_ref=columns(part, source),
            send_sem=send3.at[part, peer],
            recv_sem=recv3.at[part, source],
            device_id={
                "band": group_of(axis, quarter // 2, own(axis)[1], lax.rem(quarter, 2)),
                "gslab": lax.rem(peer, slabs),
            },
            device_id_type=MESH,
        )

    def keep(part):
        here = here_of(part % 2)
        return pltpu.make_async_copy(done.at[part, here], columns(part, here), recv3.at[part, here])

    def finish(part):
        axis = part % 2
        cross(part).wait_recv()
        for peer in range(peers):
            rows = slice(peer * mine, (peer + 1) * mine)
            done[part, peer] = (half[part, 1, rows] + came[part, rows]) * scale[axis, rows, :1]
        keep(part).start()
        here = here_of(axis)

        @pl.loop(1, peers)
        def _(k):
            deliver(part, lax.rem(here + k, peers), here).start()

    pl.semaphore_wait(barrier, devices - 1)
    send_partial(0)

    for axis in range(2):
        along, other = own(axis)
        shape = (2 * peers * mine, 1)
        tall = lax.broadcasted_iota(jnp.int32, shape, 0)
        stays = tall // (peers * mine)
        rest = lax.rem(tall, peers * mine)
        peer = rest // mine
        quarter = peer // slabs
        side = jnp.where(stays == 1, other, 1 - other)
        group = group_of(axis, quarter // 2, side, lax.rem(quarter, 2))
        output_row = (group * slabs + lax.rem(peer, slabs)) * mine + lax.rem(rest, mine)
        block = output_row // per_slice
        target = jnp.zeros(shape, jnp.int32)
        for s in range(slices):
            target = jnp.where(block == s, owner_ref[s], target)
        breadth = jnp.ones(shape, jnp.int32)
        for s in range(slices):
            breadth = jnp.where(target == s, widths_ref[s], breadth)
        root = 1.0 / jnp.sqrt(breadth.astype(jnp.float32))
        scale[axis] = jnp.broadcast_to(root[peers * mine:], (peers * mine, LANES))
        wanted = target * per_slice + lax.rem(output_row, per_slice)
        wide = lax.broadcasted_iota(jnp.int32, (1, 4 * packed), 1)
        place = lax.rem(wide, packed)
        quarter = wide // packed
        begin = group_of(axis, quarter // 2, other, lax.rem(quarter, 2)) * local_bands
        lowest = jnp.zeros((1, 4 * packed), jnp.int32)
        for s in range(slices):
            lowest = lowest + jnp.where(begin >= ends[s], 1, 0)
        offered = jnp.where(place < live, lowest * per_slice + place, -2)
        chosen[axis] = jnp.where(wanted == offered, 1.0, 0.0).astype(jnp.bfloat16)

    for step in range(1, pieces + FINISH_LAG):
        if step < pieces:
            send_partial(step)
        if 0 <= step - MERGE_LAG < pieces:
            merge(step - MERGE_LAG)
        if 0 <= step - FINISH_LAG < pieces:
            finish(step - FINISH_LAG)

    for part in range(pieces):
        cross(part).wait_send()
        here = own(part % 2)[0] * 2 + my_core

        @pl.loop(0, 3)
        def _(k):
            exchange(part, quarter_at(part % 2, k), here).wait_send()

        here = here_of(part % 2)

        @pl.loop(1, peers)
        def _(k):
            peer = lax.rem(here + k, peers)
            deliver(part, peer, peer).wait()

        keep(part).wait()


def on_device(groups, slabs, band_coeffs, sign_table, slice_widths, owner_map):
    local_bands, local_columns = band_coeffs.shape
    per_slice = sign_table.shape[0]
    rows = owner_map.shape[0] * per_slice
    share, odd = divmod(local_columns, 4 * LANES)
    if groups != 8 or odd or rows % (8 * slabs):
        return dense(band_coeffs, sign_table, slice_widths, owner_map)
    pieces = next(p for p in PIECES if share % p == 0)
    width = share // pieces * LANES
    reach = (local_bands - 2) // NARROWEST + 2
    packed = -(-reach * per_slice // 8) * 8
    mine = rows // (8 * slabs)
    peers = 4 * slabs
    return pl.pallas_call(
        functools.partial(kernel, slabs, pieces, reach),
        out_shape=jax.ShapeDtypeStruct((mine, local_columns * slabs), jnp.float32),
        in_specs=[
            pl.BlockSpec(memory_space=pltpu.SMEM),
            pl.BlockSpec(memory_space=pltpu.SMEM),
            pl.BlockSpec(memory_space=pltpu.VMEM),
            pl.BlockSpec(memory_space=pl.ANY),
        ],
        out_specs=pl.BlockSpec(memory_space=pl.ANY),
        scratch_shapes=[
            pltpu.VMEM((4 * pieces, local_bands, width), jnp.float32),
            pltpu.VMEM((packed, local_bands), jnp.bfloat16),
            pltpu.VMEM((pieces, 4, packed, width), jnp.float32),
            pltpu.VMEM((pieces, 4, packed, width), jnp.float32),
            pltpu.VMEM((2, 2 * peers * mine, 4 * packed), jnp.bfloat16),
            pltpu.VMEM((2, peers * mine, LANES), jnp.float32),
            pltpu.VMEM((pieces, 2, peers * mine, width), jnp.float32),
            pltpu.VMEM((pieces, peers * mine, width), jnp.float32),
            pltpu.VMEM((pieces, peers, mine, width), jnp.float32),
            pltpu.SemaphoreType.DMA((4 * pieces,)),
            pltpu.SemaphoreType.DMA((pieces, 4)),
            pltpu.SemaphoreType.DMA((pieces, 4)),
            pltpu.SemaphoreType.DMA((pieces,)),
            pltpu.SemaphoreType.DMA((pieces,)),
            pltpu.SemaphoreType.DMA((pieces, peers)),
            pltpu.SemaphoreType.DMA((pieces, peers)),
        ],
        compiler_params=pltpu.CompilerParams(
            collective_id=0, has_side_effects=True, vmem_limit_bytes=60 * 2**20
        ),
        name="pseudobands",
    )(slice_widths, owner_map, sign_table, band_coeffs)


def solution(mesh):
    return jax.shard_map(
        functools.partial(on_device, mesh.shape["band"], mesh.shape["gslab"]),
        mesh=mesh,
        in_specs=(P("band", "gslab"), P(None, "band"), P(), P()),
        out_specs=P(("band", "gslab"), None),
        check_vma=False,
    )
```
